1024 devices in a mesh: dp: 128 (over x, z, y_hi), tensor: 8 (over y_lo, core).
Axes of the slice: x: 4, y: 8 (y_hi: 2, y_lo: 4; y = y_hi * 4 + y_lo), z: 16, core: 2. Of those that a mesh axis runs over, the one named last changes fastest.
Arguments:
- residual: bfloat16 [2, 8192, 5120], P(None, 'dp'), may hold values from -6 to 6
- context: bfloat16 [2, 8192, 3072], P(None, 'dp', 'tensor'), may hold values from -24 to 24
- w_out: bfloat16 [3072, 5120], P('tensor'), may hold values from -0.109375 to 0.109375
- gain: float32 [5120], replicated, may hold values from 0.1 to 1.9
- cotangent: bfloat16 [2, 8192, 5120], P(None, 'dp'), may hold values from -6 to 6
- slot_rows: int32 [8, 32], P('tensor'), may hold values from 0 to 383, as said below
Outputs:
- grad_slots: float32 [8, 5120, 32], P('tensor', 'dp')
- ctx_grad: bfloat16 [2, 8192, 3072], P(None, 'dp', 'tensor')
- resid_grad: bfloat16 [2, 8192, 5120], P(None, 'dp')
The draws below stay inside these ranges and needn't reach their ends.
Inputs may be any that keep to these rules, and one draw needn't show every extreme that they name: Each row of slot_rows holds 32 different numbers.
All inputs are finite; a program needn't handle non-finite values.
Results may differ from the reference program's by a relative error of at most 0.006.
Values may be sent and summed in bfloat16 or wider, within the bound.
No kernel may reach another device: no remote copies, remote signals or barrier semaphores. Data moves between devices by JAX's collectives and lax.ppermute only.
A program may use at most 64 MiB of HBM per device.

```python
import jax
import jax.numpy as jnp
from jax import lax

DW = 5120
MICRO = 2
BUCKET = 32
HD_DEV = 384
HD = 3072
GROUPS = 8
REPLICAS = 128
TOKENS = 8192


def draw_slot_rows(key, part):
    keys = jax.random.split(jax.random.fold_in(key, 7), GROUPS)
    rows = jax.vmap(lambda single: jax.random.permutation(single, HD_DEV))(keys)
    return rows[:, :BUCKET].astype(jnp.int32)


def raised(values, rng, source, target, shards_of, factor):
    owner, partner = [(jnp.arange(values.shape[position]) // (values.shape[position] // shards_of)).reshape([-1 if axis == position else 1 for axis in range(values.ndim)]) for position in (source, target)]
    chosen = jax.random.permutation(rng, shards_of)[partner]
    strong = (owner == chosen) | (owner == (partner + shards_of // 2) % shards_of)
    return jnp.where(strong, factor * values, values)


def block_levels(rng, dims, shards, least, high):
    level = 1.0
    for axis_at, shards_of in shards:
        steps = jax.random.uniform(jax.random.fold_in(jax.random.fold_in(rng, 6), axis_at), (shards_of,), jnp.float32, least / len(shards), high / len(shards))
        level = level * jnp.repeat(jnp.exp(steps), dims[axis_at] // shards_of).reshape((-1,) + (1,) * (len(dims) - 1 - axis_at))
    return level


def bell_draw(rng, shape, scale, reach, pieces=(), kind=jnp.bfloat16):
    drawn = scale * jax.random.normal(rng, shape, jnp.float32)
    if pieces:
        drawn = drawn * block_levels(rng, shape, pieces, -0.22, 0.18)
    return jnp.clip(drawn, -reach, reach).astype(kind)


def gaussian_with(key, shape, spread, limit, cuts, heavy, dtype=jnp.bfloat16):
    values = spread * jax.random.normal(key, shape, jnp.float32)
    if cuts:
        values = values * block_levels(key, shape, cuts, -0.22, 0.18)
    return jnp.clip(raised(values, jax.random.fold_in(key, 3), *heavy), -limit, limit).astype(dtype)


def setup_inputs(seed: int = 0) -> dict:
    key_of = jax.random.split(jax.random.key(seed), 7)
    return {
        "residual": bell_draw(key_of[0], (MICRO, TOKENS, DW), 1.0, 6.0, ((1, 128),)),
        "context": gaussian_with(key_of[1], (MICRO, TOKENS, HD), 1.0, 24.0, ((1, 128), (2, 8)), (1, 2, 128, 5.5)),
        "w_out": bell_draw(key_of[2], (HD, DW), HD ** -0.5, 0.109375, ((0, 8),)),
        "gain": jnp.clip(1.0 + 0.18 * jax.random.normal(key_of[3], (DW,), jnp.float32), 0.1, 1.9),
        "cotangent": bell_draw(key_of[4], (MICRO, TOKENS, DW), 1.0, 6.0, ((1, 128),)),
        "slot_rows": draw_slot_rows(jax.random.fold_in(key_of[6], 71), 0),
    }


def norm_backward(res_rows, summed, gain, cot_rows):
    hidden = res_rows.astype(jnp.float32) + summed
    center = hidden - lax.optimization_barrier(jnp.mean(hidden, axis=-1, keepdims=True))
    inverse = lax.rsqrt(lax.optimization_barrier(jnp.mean(center * center, axis=-1, keepdims=True)) + 1e-05)
    normed = center * inverse
    upstream = cot_rows.astype(jnp.float32) * gain
    result = inverse * (upstream - lax.optimization_barrier(jnp.mean(upstream, axis=-1, keepdims=True)) - normed * lax.optimization_barrier(jnp.mean(upstream * normed, axis=-1, keepdims=True)))
    return result.astype(jnp.bfloat16)

def reference(residual, context, w_out, gain, cotangent, slot_rows):
    groups = slot_rows.shape[0]
    width = w_out.shape[0] // groups
    gradient = jnp.zeros((w_out.shape[0], w_out.shape[1]), jnp.float32)
    resid_list = []
    ctx_list = []
    for micro_idx in range(residual.shape[0]):
        ctx_rows = context[micro_idx]
        summed = jnp.zeros(residual.shape[1:], jnp.float32)
        for group_idx in range(groups):
            first_row = group_idx * width
            partial_value = jnp.dot(ctx_rows[:, first_row:first_row + width], w_out[first_row:first_row + width], preferred_element_type=jnp.float32)
            summed = summed + lax.optimization_barrier(partial_value.astype(jnp.bfloat16)).astype(jnp.float32)
        grad_rows = norm_backward(residual[micro_idx], summed, gain, cotangent[micro_idx])
        resid_list.append(grad_rows)
        ctx_back = lax.dot_general(grad_rows, w_out, (((1,), (1,)), ((), ())), preferred_element_type=jnp.float32)
        ctx_list.append(ctx_back.astype(jnp.bfloat16))
        gradient = gradient + lax.dot_general(ctx_rows, grad_rows, (((0,), (0,)), ((), ())), preferred_element_type=jnp.float32)
    gradient = gradient / REPLICAS
    slots = jnp.take_along_axis(gradient.reshape(groups, width, -1), slot_rows[:, :, None], axis=1)
    return (jnp.transpose(slots, (0, 2, 1)), jnp.stack(ctx_list), jnp.stack(resid_list))
```

```python
import jax
import jax.numpy as jnp
from jax import lax
from jax.sharding import Mesh
from jax.sharding import PartitionSpec as P

DP = ("x", "z", "yh")
TENSOR = ("yl", "core")
SHAPE = (4, 16, 2, 4, 2)
BF16, F32 = jnp.bfloat16, jnp.float32


def shifted(array, axis, step):
    n = lax.axis_size(axis)
    return lax.ppermute(array, axis, [(i, (i + step) % n) for i in range(n)])


def norm_backward(hidden, gain, cot_rows):
    center = hidden - jnp.mean(hidden, axis=-1, keepdims=True)
    inverse = lax.rsqrt(jnp.mean(center * center, axis=-1, keepdims=True) + 1e-05)
    normed = center * inverse
    upstream = cot_rows.astype(F32) * gain
    result = inverse * (
        upstream
        - jnp.mean(upstream, axis=-1, keepdims=True)
        - normed * jnp.mean(upstream * normed, axis=-1, keepdims=True)
    )
    return result.astype(BF16)


def body(residual, context, w_out, gain, cotangent, slot_rows):
    micros, tokens, width = residual.shape
    heads = context.shape[-1]
    chips, cores = lax.axis_size("yl"), lax.axis_size("core")
    core, chip = lax.axis_index("core"), lax.axis_index("yl")
    rows = tokens // (chips * cores)
    share = micros * rows

    def half(array, which):
        blocks = array.reshape(micros, cores, chips, rows, array.shape[-1])
        picked = lax.dynamic_index_in_dim(blocks, which, 1, keepdims=False)
        return jnp.swapaxes(picked, 0, 1).reshape(chips * share, array.shape[-1])

    mine, theirs = half(context, core), half(context, 1 - core)
    order = slot_rows[0]

    sent = jnp.dot(theirs, w_out, preferred_element_type=F32).astype(BF16)
    received = shifted(sent, "core", 1)
    summed = jnp.dot(mine, w_out, preferred_element_type=F32) + received.astype(F32)

    def piece(array, at):
        return lax.dynamic_slice_in_dim(array, (at % chips) * share, share, 0)

    rounded = summed.astype(BF16)
    parts = [
        shifted(piece(rounded, chip + step), "yl", step) for step in range(1, chips)
    ]
    first = (core * chips + chip) * rows
    res_rows = lax.dynamic_slice_in_dim(residual, first, rows, 1).reshape(share, width)
    cot_rows = lax.dynamic_slice_in_dim(cotangent, first, rows, 1).reshape(share, width)
    hidden = res_rows.astype(F32) + piece(summed, chip)
    for part in parts:
        hidden = hidden + part.astype(F32)
    grad = norm_backward(hidden, gain, cot_rows)

    mine_grad = lax.all_gather(grad, "yl", axis=0, tiled=True)
    their_grad = shifted(mine_grad, "core", 1)

    def bucket(ctx, rows_grad):
        return lax.dot_general(
            jnp.take(ctx, order, axis=1),
            rows_grad,
            (((0,), (0,)), ((), ())),
            preferred_element_type=F32,
        )

    gradient = bucket(mine, mine_grad) + bucket(theirs, their_grad)
    slots = gradient.shape[0]
    nx, nzy = lax.axis_size("x"), lax.axis_size(("z", "yh"))
    by_x = jnp.swapaxes(gradient.astype(BF16).reshape(slots, nx, width // nx), 0, 1)
    by_x = lax.all_to_all(by_x, "x", 0, 0, tiled=True)
    plane = jnp.sum(by_x.astype(F32), axis=0).astype(BF16)
    by_zy = jnp.swapaxes(plane.reshape(slots, nzy, width // (nx * nzy)), 0, 1)
    by_zy = lax.all_to_all(by_zy, ("z", "yh"), 0, 0, tiled=True)
    reduced = jnp.sum(by_zy.astype(F32), axis=0) / lax.axis_size(DP)

    def whole(own, other):
        low = jnp.where(core == 0, own, other)
        high = jnp.where(core == 0, other, own)
        both = jnp.stack([low, high]).reshape(cores, chips, micros, rows, -1)
        return jnp.transpose(both, (2, 0, 1, 3, 4)).reshape(micros, tokens, -1)

    def back(rows_grad):
        return lax.dot_general(
            rows_grad, w_out, (((1,), (1,)), ((), ())), preferred_element_type=F32
        ).astype(BF16)

    ctx_grad = whole(back(mine_grad), back(their_grad))
    return (reduced.T[None], ctx_grad, whole(mine_grad, their_grad))


def solution(mesh):
    split = Mesh(mesh.devices.reshape(SHAPE), DP + TENSOR)
    in_specs = (
        P(None, DP, None),
        P(None, DP, TENSOR),
        P(TENSOR, None),
        P(),
        P(None, DP, None),
        P(TENSOR, None),
    )
    out_specs = (P(TENSOR, DP, None), P(None, DP, TENSOR), P(None, DP, None))
    return jax.shard_map(body, mesh=split, in_specs=in_specs, out_specs=out_specs, check_vma=False)
```
